512 devices in a mesh: rep: 64 (over z, x), shard: 8 (over y, core).
Axes of the slice: x: 4, y: 4, z: 16, core: 2. Of those that a mesh axis runs over, the one named last changes fastest.
Arguments:
- outer_params: float32 [16, 131072], P('shard'), may hold values from -6 to 6
- replica_delta: float32 [64, 16, 131072], P('rep', 'shard'), may hold values from -20 to 20
- momentum: float32 [16, 131072], P('shard', 'rep'), may hold values from -20 to 20
- tensor_of_block: int32 [16], P('shard'), may hold values from 0 to 3, as said below
Outputs:
- new_params: float32 [16, 131072], P('shard')
- new_momentum: float32 [16, 131072], P('shard', 'rep')
The draws below stay inside these ranges and needn't reach their ends.
Inputs may be any that keep to these rules, and one draw needn't show every extreme that they name: `tensor_of_block`: every tensor owns exactly 4 blocks.
All inputs are finite; a program needn't handle non-finite values.
Results may differ from the reference program's by a relative error of at most 0.00028.
Values sent between devices are 32-bit elements; how exact they have to be, the bound alone decides.
A program may use at most 64 MiB of HBM per device.

```python
import math
import jax
import jax.numpy as jnp
from jax import lax

BLOCK_ROWS = 128
BLOCK_COLS = 1024
NS_STEPS = 8
REPLICAS = 64
BLOCKS = 16
GROUPS = 4


def common_parts(key):
    base = jax.random.fold_in(key, 11)
    log_scale = jax.random.uniform(jax.random.fold_in(base, 1), (BLOCKS, 1), jnp.float32, math.log(0.5), math.log(2.0))
    shared = jnp.clip(jax.random.normal(jax.random.fold_in(base, 2), (BLOCKS, BLOCK_ROWS * BLOCK_COLS), jnp.float32), -5.0, 5.0)
    align = jax.random.uniform(jax.random.fold_in(base, 3), (BLOCKS, 1), jnp.float32, -1.0, 1.0)
    return (jnp.exp(log_scale), shared, align)


def draw_momentum(key, part):
    scale, shared, align = common_parts(key)
    noise = jnp.clip(jax.random.normal(jax.random.fold_in(key, 21), shared.shape, jnp.float32), -5.0, 5.0)
    values = 0.7 * scale * (align * shared + noise)
    return values.astype(jnp.float32)


def draw_replica_delta(key, part):
    scale, shared, align = common_parts(key)
    noise = jnp.clip(jax.random.normal(jax.random.fold_in(key, 31), (REPLICAS, BLOCKS, BLOCK_ROWS * BLOCK_COLS), jnp.float32), -5.0, 5.0)
    values = scale[None] * (shared[None] + noise)
    return values.astype(jnp.float32)


def draw_tensor_of_block(key, part):
    order = jax.random.permutation(jax.random.fold_in(key, 41), BLOCKS)
    return (order % GROUPS).astype(jnp.int32)


def block_levels(stream_key, shape, shards, least, high):
    def one(position, shards_of):
        steps = jax.random.uniform(jax.random.fold_in(jax.random.fold_in(stream_key, 6), position), (shards_of,), jnp.float32, least / len(shards), high / len(shards))
        return jnp.repeat(jnp.exp(steps), shape[position] // shards_of).reshape((-1,) + (1,) * (len(shape) - position - 1))

    factor_of = one(*shards[0])
    for cut in shards[1:]:
        factor_of = factor_of * one(*cut)
    return factor_of


def gaussian(key, extent, scale, reach, split=(), held_as=jnp.bfloat16):
    drawn = jax.random.normal(key, extent, jnp.float32) * scale
    if len(split) > 0:
        drawn = block_levels(key, extent, split, -0.22, 0.18) * drawn
    return jnp.clip(drawn, min=-reach, max=reach).astype(held_as)


def setup_inputs(seed: int = 0) -> dict:
    seeds = jax.random.split(jax.random.key(seed), 5)
    return {
        "outer_params": gaussian(seeds[0], (BLOCKS, BLOCK_ROWS * BLOCK_COLS), 1.0, 6.0, ((0, 8),), jnp.float32),
        "replica_delta": draw_replica_delta(jax.random.fold_in(seeds[4], 71), 0),
        "momentum": draw_momentum(jax.random.fold_in(seeds[4], 71), 0),
        "tensor_of_block": draw_tensor_of_block(jax.random.fold_in(seeds[4], 71), 0),
    }


outer_rate = 0.7
decay_rate = 0.9

def orthogonalize(direction):
    blocks = direction.reshape(direction.shape[0], BLOCK_ROWS, BLOCK_COLS)
    blocks = blocks / jnp.sqrt(lax.optimization_barrier(jnp.sum(blocks * blocks, axis=(1, 2), keepdims=True)) + 1.0)
    for step in range(NS_STEPS):
        square = jnp.einsum('bij,bkj->bik', blocks, blocks, precision=lax.Precision.HIGHEST)
        blocks = 1.5 * blocks - 0.5 * jnp.einsum('bik,bkj->bij', square, blocks, precision=lax.Precision.HIGHEST)
    return blocks.reshape(direction.shape[0], BLOCK_ROWS * BLOCK_COLS)

def reference(outer_params, replica_delta, momentum, tensor_of_block):
    mean_delta = lax.optimization_barrier(jnp.sum(replica_delta, axis=0)) / REPLICAS
    new_momentum = decay_rate * momentum + mean_delta
    direction = mean_delta + decay_rate * new_momentum
    update = orthogonalize(direction)
    member = (tensor_of_block[:, None] == jnp.arange(GROUPS, dtype=jnp.int32)[None, :]).astype(jnp.float32)
    per_block = jnp.stack([lax.optimization_barrier(jnp.sum(outer_params * outer_params, axis=1)), lax.optimization_barrier(jnp.sum(update * update, axis=1))], axis=1)
    tensor_sums = lax.optimization_barrier(jnp.sum(member[:, :, None] * per_block[:, None, :], axis=0))
    group_rate = outer_rate * jnp.sqrt(jnp.maximum(tensor_sums[:, 0], 1.0) / jnp.maximum(tensor_sums[:, 1], 1.0))
    block_rate = lax.optimization_barrier(jnp.sum(member * group_rate[None, :], axis=1))
    new_params = outer_params - block_rate[:, None] * update
    return (new_params, new_momentum)
```

```python
import jax
import jax.numpy as jnp
from jax import lax
from jax.experimental import pallas as pl
from jax.experimental.pallas import tpu as pltpu
from jax.sharding import Mesh
from jax.sharding import PartitionSpec as P

NZ, NX, NY, NC = 16, 4, 4, 2
CH = 32
HF = CH // 2
ROWS = NZ * NX * CH
NS_STEPS = 8
LEAD = 5
RATE = 0.7
DECAY = 0.9
MESH = pl.DeviceIdType.MESH
HI = lax.Precision.HIGHEST
F32 = jnp.float32

OFFS = [8, 7, -7, 6, -6, 5, -5, 4, -4, 3, -3, 2, -2, 1, -1, 0]
AOFFS = [0, 1, -1, 2, -2, 3, -3, 4, -4, 5, -5, 6, -6, 7, -7, 8]


def kernel(
    tob_ref, params_h, delta_h, mom_h, out_v, newm_v,
    params_v, delta_v, mom_v, dir_v, xm_v,
    ra_v, as_v, rc_v, zs_v, rel_v, zr_v, u_v, sums_v,
    lsem,
    ra_sem, rc_sem, rel_sem, zr_sem, ag_sem, agh_sem, xf_sem, xh_sem, sum_sem,
    sa_sem, sb_sem, sc_sem, sz_sem, sagz_sem, sagzh_sem, sxf_sem, sxh_sem, ssum_sem,
):
    z, x = lax.axis_index("z"), lax.axis_index("x")
    y, c = lax.axis_index("y"), lax.axis_index("core")
    zo = lambda o: lax.rem(z + (o + 2 * NZ), NZ)
    xo = lambda o: lax.rem(x + (o + 2 * NX), NX)
    row = lambda zz, xx, off=0: pl.multiple_of((zz * NX + xx) * CH + off, HF)

    def rdma(src, dst, ssem, rsem, dev):
        return pltpu.make_async_remote_copy(
            src_ref=src, dst_ref=dst, send_sem=ssem, recv_sem=rsem,
            device_id=dev, device_id_type=MESH,
        )

    loads = [
        pltpu.make_async_copy(delta_h, delta_v, lsem.at[0]),
        pltpu.make_async_copy(params_h, params_v, lsem.at[1]),
        pltpu.make_async_copy(mom_h, mom_v, lsem.at[2]),
    ]
    for cp in loads:
        cp.start()

    barrier = pltpu.get_barrier_semaphore()
    count = 0
    for o in (1, -1):
        pl.semaphore_signal(barrier, inc=1, device_id={"x": xo(o)}, device_id_type=MESH)
        count += 1
    for o in (1, -1, 2, -2, 3, -3, 4, -4):
        pl.semaphore_signal(barrier, inc=1, device_id={"z": zo(o)}, device_id_type=MESH)
        count += 1
    shard_peers = []
    for k in range(1, NY * NC):
        me = y * NC + c
        other = lax.rem(me + k, NY * NC)
        shard_peers.append({"y": other // NC, "core": lax.rem(other, NC)})
    for dev in shard_peers:
        pl.semaphore_signal(barrier, inc=1, device_id=dev, device_id_type=MESH)
        count += 1
    loads[0].wait()
    pl.semaphore_wait(barrier, count)

    def send_a(s):
        zd = zo(OFFS[s])
        for d, sg in ((0, 1), (1, -1)):
            src = delta_v.at[pl.ds(row(zd, xo(2), d * HF), HF), :]
            rdma(src, ra_v.at[d, s], sa_sem.at[d], ra_sem.at[d, s], {"x": xo(sg)}).start()

    def send_bc(s):
        zd = zo(OFFS[s])
        for d, sg in ((0, 1), (1, -1)):
            rdma(ra_v.at[d, s], ra_v.at[d, s], sa_sem.at[d], ra_sem.at[d, s], {"x": xo(sg)}).wait_recv()
            own = delta_v[pl.ds(row(zd, xo(sg), d * HF), HF), :]
            as_v[d, s] = own + ra_v[d, s]
        for d, sg in ((0, 1), (1, -1)):
            src = delta_v.at[pl.ds(row(zd, xo(sg), (1 - d) * HF), HF), :]
            dst = rc_v.at[d, s, pl.ds((1 - d) * HF, HF), :]
            rdma(src, dst, sb_sem.at[d], rc_sem.at[d, s], {"x": xo(sg)}).start()
        for d, sg in ((0, 1), (1, -1)):
            dst = rc_v.at[d, s, pl.ds(d * HF, HF), :]
            rdma(as_v.at[d, s], dst, sc_sem.at[d], rc_sem.at[d, s], {"x": xo(sg)}).start()

    def x_total(s):
        zd = zo(OFFS[s])
        for d, sg in ((0, 1), (1, -1)):
            rdma(rc_v.at[d, s], rc_v.at[d, s], sc_sem.at[d], rc_sem.at[d, s], {"x": xo(sg)}).wait_recv()
        return delta_v[pl.ds(row(zd, x), CH), :] + rc_v[0, s] + rc_v[1, s]

    def z_send(s):
        o = OFFS[s]
        t = x_total(s)
        if o == 0:
            zs_v[s] = t
        elif o == 8:
            zs_v[s] = t
            for d, sg in ((0, 1), (1, -1)):
                h = pl.ds(d * HF, HF)
                rdma(zs_v.at[s, h, :], rel_v.at[d, 3, h, :], sz_sem.at[s, d], rel_sem.at[d, 3], {"z": zo(4 * sg)}).start()
        elif abs(o) > 4:
            zs_v[s] = t
            d, sg = (0, 1) if o > 0 else (1, -1)
            k = abs(o) - 4
            rdma(zs_v.at[s], rel_v.at[d, k - 1], sz_sem.at[s, 0], rel_sem.at[d, k - 1], {"z": zo(k * sg)}).start()
        else:
            d, sg = (0, 1) if o > 0 else (1, -1)
            if abs(o) == 4:
                for k in (1, 2, 3):
                    rdma(rel_v.at[d, k - 1], rel_v.at[d, k - 1], sz_sem.at[s, 0], rel_sem.at[d, k - 1], {"z": zo(k * sg)}).wait_recv()
                    t = t + rel_v[d, k - 1]
                h = pl.ds(d * HF, HF)
                rdma(rel_v.at[d, 3, h, :], rel_v.at[d, 3, h, :], sz_sem.at[s, 0], rel_sem.at[d, 3], {"z": zo(4 * sg)}).wait_recv()
                zs_v[s] = t
                zs_v[s, h, :] = zs_v[s, h, :] + rel_v[d, 3, h, :]
            else:
                zs_v[s] = t
            k = abs(o)
            rdma(zs_v.at[s], zr_v.at[d, k - 1], sz_sem.at[s, 0], zr_sem.at[d, k - 1], {"z": zo(k * sg)}).start()

    for s in range(LEAD):
        send_a(s)
    loads[1].wait()
    p2 = []
    for b in range(2):
        part = params_v[pl.ds(b, ROWS // 2, stride=2), :]
        part = jnp.sum((part * part).reshape(ROWS // 16, 8, 128), axis=0)
        p2.append(jnp.sum(jnp.sum(part, axis=0, keepdims=True), axis=1, keepdims=True))
    for s in range(NZ + LEAD):
        if s + LEAD < NZ:
            send_a(s + LEAD)
        if s < NZ:
            send_bc(s)
        if s >= LEAD:
            z_send(s - LEAD)

    total = zs_v[NZ - 1]
    for k in (1, 2, 3, 4):
        for d, sg in ((0, 1), (1, -1)):
            rdma(zr_v.at[d, k - 1], zr_v.at[d, k - 1], sz_sem.at[0, 0], zr_sem.at[d, k - 1], {"z": zo(k * sg)}).wait_recv()
            total = total + zr_v[d, k - 1]
    loads[2].wait()
    mean = total * (1.0 / 64.0)
    newm = DECAY * mom_v[...] + mean
    own = pl.ds(row(z, x), CH)
    dir_v[own, :] = mean + DECAY * newm
    newm_v[...] = newm

    def ag_z(src_o, k, sg, half=None):
        at = row(zo(src_o), x)
        r = pl.ds(at, CH) if half is None else pl.ds(pl.multiple_of(at + half * HF, HF), HF)
        dest_o = (src_o - k * sg + 8) % NZ - 8
        if half is None:
            rsem, ssem = ag_sem.at[dest_o + 8], sagz_sem.at[src_o + 8, (0 if sg > 0 else 1), k - 1]
        else:
            rsem, ssem = agh_sem.at[half], sagzh_sem.at[half]
        ref = dir_v.at[r, :]
        return rdma(ref, ref, ssem, rsem, {"z": zo(k * sg)})

    sends = []

    def go(cp):
        cp.start()
        sends.append(cp)

    for k in (4, 1, 2, 3):
        for sg in (1, -1):
            go(ag_z(0, k, sg))

    def wait_z(o):
        if o == 8:
            for h in range(2):
                ref = dir_v.at[pl.ds(row(zo(8), x, h * HF), HF), :]
                rdma(ref, ref, sagzh_sem.at[h], agh_sem.at[h], {"z": zo(1)}).wait_recv()
        elif o != 0:
            ref = dir_v.at[pl.ds(row(zo(o), x), CH), :]
            rdma(ref, ref, sagzh_sem.at[0], ag_sem.at[(o + 8) % NZ], {"z": zo(1)}).wait_recv()

    def x_first(i):
        o = AOFFS[i]
        wait_z(o)
        if o == -4:
            for k in (4, 3, 2, 1):
                go(ag_z(o, k, 1, 0 if k == 4 else None))
        if o == 4:
            for k in (4, 3, 2, 1):
                go(ag_z(o, k, -1, 1 if k == 4 else None))
        ref = dir_v.at[pl.ds(row(zo(o), x), CH), :]
        for d, sg in ((0, 1), (1, -1)):
            rdma(ref, ref, sxf_sem.at[d], xf_sem.at[d, i], {"x": xo(sg)}).start()

    def x_second(i):
        o = AOFFS[i]
        for d, sg in ((0, 1), (1, -1)):
            ref = dir_v.at[pl.ds(row(zo(o), xo(-sg)), CH), :]
            rdma(ref, ref, sxf_sem.at[d], xf_sem.at[d, i], {"x": xo(sg)}).wait_recv()
            half = dir_v.at[pl.ds(row(zo(o), xo(-sg), d * HF), HF), :]
            rdma(half, half, sxh_sem.at[d], xh_sem.at[d, i], {"x": xo(sg)}).start()

    def relayout(i):
        o = AOFFS[i]
        for d, sg in ((0, 1), (1, -1)):
            half = dir_v.at[pl.ds(row(zo(o), xo(2), d * HF), HF), :]
            rdma(half, half, sxh_sem.at[d], xh_sem.at[d, i], {"x": xo(sg)}).wait_recv()
        base = zo(o) * (NX * CH)
        rows8 = pl.ds(pl.multiple_of(zo(o) * 8, 8), 8)
        for b in range(2):
            for j in range(8):
                xm_v[b, rows8, j * 128 : (j + 1) * 128] = dir_v[pl.ds(base + j * 2 + b, 8, stride=16), :]

    LAG = 3
    for i in range(NZ + 2 * LAG):
        if i < NZ:
            x_first(i)
        if LAG <= i < NZ + LAG:
            x_second(i - LAG)
        if i >= 2 * LAG:
            relayout(i - 2 * LAG)

    r = lax.broadcasted_iota(jnp.int32, (128, 128), 0)
    q = lax.broadcasted_iota(jnp.int32, (128, 128), 1)
    eye = (r == q).astype(F32)

    def all_sum(v):
        return jnp.sum(jnp.sum(v, axis=0, keepdims=True), axis=1, keepdims=True)

    def mm(a, b):
        return jnp.dot(a, b, precision=HI, preferred_element_type=F32)

    grams, scales, prods = [], [], [None, None]
    for b in range(2):
        xb = xm_v[b]
        gram = lax.dot_general(xb, xb, (((1,), (1,)), ((), ())), precision=HI, preferred_element_type=F32)
        norm = all_sum(gram * eye) + 1.0
        grams.append(gram / norm)
        scales.append(lax.rsqrt(norm))
    u2 = [None, None]
    for step in range(NS_STEPS):
        for b in range(2):
            m = 1.5 * eye - 0.5 * grams[b]
            t = mm(grams[b], m)
            prods[b] = m if step == 0 else mm(m, prods[b])
            if step < NS_STEPS - 1:
                grams[b] = mm(t, m)
            else:
                u2[b] = all_sum(t * m)

    rr = lax.broadcasted_iota(jnp.int32, (8, 128), 0)
    qq = lax.broadcasted_iota(jnp.int32, (8, 128), 1)
    tile = jnp.zeros((8, 128), F32)
    for b in range(2):
        mine = rr == tob_ref[b]
        tile = tile + jnp.where(mine & (qq == 0), p2[b], 0.0) + jnp.where(mine & (qq == 1), u2[b], 0.0)
    me = y * NC + c
    sums_v[me] = tile
    for k, dev in enumerate(shard_peers):
        cp = rdma(sums_v.at[me], sums_v.at[me], ssum_sem.at[k], sum_sem.at[6 - k], dev)
        go(cp)
    for b in range(2):
        u_v[b] = mm(prods[b] * scales[b], xm_v[b])
    for k in range(NY * NC - 1):
        other = lax.rem(me + k + 1, NY * NC)
        rdma(sums_v.at[other], sums_v.at[other], ssum_sem.at[k], sum_sem.at[k], shard_peers[k]).wait_recv()
    sums = sums_v[0]
    for k in range(1, NY * NC):
        sums = sums + sums_v[k]
    sums = jnp.maximum(sums, 1.0)
    for b in range(2):
        mine = rr == tob_ref[b]
        num = all_sum(jnp.where(mine & (qq == 0), sums, 0.0))
        den = all_sum(jnp.where(mine & (qq == 1), sums, 0.0))
        rate = RATE * jnp.sqrt(num / den)
        for j in range(8):
            at = pl.ds(j * 2 + b, 128, stride=16)
            out_v[at, :] = params_v[at, :] - rate * u_v[b, :, j * 128 : (j + 1) * 128]

    for d in range(2):
        n = NZ * HF
        for sem in (sa_sem, sb_sem, sc_sem, sxh_sem):
            ref = delta_v.at[pl.ds(0, n), :]
            rdma(ref, ref, sem.at[d], rc_sem.at[d, 0], {"x": xo(1)}).wait_send()
        ref = delta_v.at[pl.ds(0, NZ * CH), :]
        rdma(ref, ref, sxf_sem.at[d], rc_sem.at[d, 0], {"x": xo(1)}).wait_send()
    for s in range(NZ - 1):
        if OFFS[s] == 8:
            for d in range(2):
                h = pl.ds(d * HF, HF)
                rdma(zs_v.at[s, h, :], zs_v.at[s, h, :], sz_sem.at[s, d], rel_sem.at[d, 3], {"z": zo(1)}).wait_send()
        else:
            rdma(zs_v.at[s], zs_v.at[s], sz_sem.at[s, 0], rel_sem.at[0, 0], {"z": zo(1)}).wait_send()
    for cp in sends:
        cp.wait_send()


def shards(outer_params, replica_delta, momentum, tensor_of_block):
    def rows_of(array, blocks=2):
        return array.reshape(blocks, -1, 128).transpose(1, 0, 2).reshape(-1, 128)

    def cols_of(array, blocks=2):
        return array.reshape(-1, blocks, 128).transpose(1, 0, 2).reshape(blocks, -1)

    params, delta, mom = rows_of(outer_params), rows_of(replica_delta[0]), rows_of(momentum)
    dma, vmem = pltpu.SemaphoreType.DMA, pltpu.VMEM
    new_params, new_momentum = pl.pallas_call(
        kernel,
        out_shape=(
            jax.ShapeDtypeStruct(params.shape, F32),
            jax.ShapeDtypeStruct(mom.shape, F32),
        ),
        in_specs=[pl.BlockSpec(memory_space=pltpu.SMEM)] + [pl.BlockSpec(memory_space=pltpu.HBM)] * 3,
        out_specs=[pl.BlockSpec(memory_space=pltpu.VMEM)] * 2,
        scratch_shapes=[
            vmem((ROWS, 128), F32), vmem((ROWS, 128), F32), vmem((CH, 128), F32),
            vmem((ROWS, 128), F32), vmem((2, 128, 1024), F32),
            vmem((2, NZ, HF, 128), F32), vmem((2, NZ, HF, 128), F32), vmem((2, NZ, CH, 128), F32),
            vmem((NZ, CH, 128), F32), vmem((2, 4, CH, 128), F32), vmem((2, 4, CH, 128), F32),
            vmem((2, 128, 1024), F32), vmem((8, 8, 128), F32),
            dma((3,)),
            dma((2, NZ)), dma((2, NZ)), dma((2, 4)), dma((2, 4)), dma((NZ,)), dma((2,)),
            dma((2, NZ)), dma((2, NZ)), dma((7,)),
            dma((2,)), dma((2,)), dma((2,)), dma((NZ, 2)), dma((NZ, 2, 4)), dma((2,)),
            dma((2,)), dma((2,)), dma((7,)),
        ],
        compiler_params=pltpu.CompilerParams(
            collective_id=0, has_side_effects=True, vmem_limit_bytes=40 * 1024 * 1024
        ),
    )(tensor_of_block, params, delta, mom)
    return (cols_of(new_params), cols_of(new_momentum))


def solution(mesh):
    finer = Mesh(mesh.devices.reshape(NZ, NX, NY, NC), ("z", "x", "y", "core"))
    rep, shard = ("z", "x"), ("y", "core")
    in_specs = (P(shard, None), P(rep, shard, None), P(shard, rep), P(shard))
    out_specs = (P(shard, None), P(shard, rep))
    return jax.shard_map(
        shards, mesh=finer, in_specs=in_specs, out_specs=out_specs, check_vma=False
    )
```
